16 devices in a mesh: ty: 4 (over z, y), tx: 4 (over x, core).
Axes of the slice: x: 2, y: 2, z: 2, core: 2. Of those that a mesh axis runs over, the one named last changes fastest.
Arguments:
- x_tok: bfloat16 [4096, 2048], P('ty', 'tx')
- dy_tok: bfloat16 [4096, 2048], P('ty', 'tx')
- ln_gain: float32 [2048], P('tx')
- w_gate: bfloat16 [2048, 8192], P('tx', 'ty')
- w_up: bfloat16 [2048, 8192], P('tx', 'ty')
- w_down: bfloat16 [8192, 2048], P('ty', 'tx')
Outputs:
- output 1: bfloat16 [4096, 2048], P('ty', 'tx')
- output 2: bfloat16 [4096, 2048], P('ty', 'tx')
- output 3: float32 [2048, 8192], P('tx', 'ty')
- output 4: float32 [2048, 8192], P('tx', 'ty')
- output 5: float32 [8192, 2048], P('ty', 'tx')
- output 6: float32 [2048], P('tx')
All inputs are finite; a program needn't handle non-finite values.
Results may differ from the reference program's by a relative error of at most 0.00118.
Values are sent between devices in bfloat16 or wider.
A program may use at most 1 GiB of HBM per device.

```python
import jax
import jax.numpy as jnp
from jax import lax

TOKENS = 4096
D_MODEL = 2048
D_FF = 8192
LN_EPS = 1e-6


def setup_inputs(seed: int = 0) -> dict:
    key_list = jax.random.split(jax.random.key(seed), 9)
    x_tok = (jax.random.normal(key_list[0], (TOKENS, D_MODEL), jnp.float32)
             + 1.5 * jax.random.normal(key_list[1], (TOKENS, 1), jnp.float32)).astype(jnp.bfloat16)
    dy_tok = jax.random.normal(key_list[2], (TOKENS, D_MODEL), jnp.float32).astype(jnp.bfloat16)
    ln_gain = 1.0 + 0.5 * jax.random.normal(key_list[3], (D_MODEL,), jnp.float32)
    in_scale = D_MODEL ** -0.5
    w_gate = ((jax.random.normal(key_list[4], (D_MODEL, D_FF), jnp.float32)
               + jax.random.normal(key_list[5], (1, D_FF), jnp.float32)) * in_scale).astype(jnp.bfloat16)
    w_up = ((jax.random.normal(key_list[6], (D_MODEL, D_FF), jnp.float32)
             + jax.random.normal(key_list[7], (1, D_FF), jnp.float32)) * in_scale).astype(jnp.bfloat16)
    w_down = (jax.random.normal(key_list[8], (D_FF, D_MODEL), jnp.float32) * D_FF ** -0.5).astype(jnp.bfloat16)
    return {"x_tok": x_tok, "dy_tok": dy_tok, "ln_gain": ln_gain,
            "w_gate": w_gate, "w_up": w_up, "w_down": w_down}


def reference(x_tok, dy_tok, ln_gain, w_gate, w_up, w_down):
    x_float = x_tok.astype(jnp.float32)
    mean_x = jnp.mean(x_float, axis=1, keepdims=True)
    mean_sq = jnp.mean(x_float * x_float, axis=1, keepdims=True)
    inv_std = lax.rsqrt(mean_sq - mean_x * mean_x + LN_EPS)
    x_hat = (x_float - mean_x) * inv_std
    h_norm = (ln_gain * x_hat).astype(jnp.bfloat16)
    gate_pre = jnp.dot(h_norm, w_gate, preferred_element_type=jnp.float32)
    up_pre = jnp.dot(h_norm, w_up, preferred_element_type=jnp.float32)
    gate_sig = jax.nn.sigmoid(gate_pre)
    gate_swish = gate_pre * gate_sig
    act_out = (gate_swish * up_pre).astype(jnp.bfloat16)
    mlp_out = jnp.dot(act_out, w_down, preferred_element_type=jnp.float32)
    y_tok = (x_float + mlp_out).astype(jnp.bfloat16)
    dw_down = jnp.dot(act_out.T, dy_tok, preferred_element_type=jnp.float32)
    d_act = jnp.dot(dy_tok, w_down.T, preferred_element_type=jnp.float32)
    d_gate = (d_act * up_pre * gate_sig * (1.0 + gate_pre * (1.0 - gate_sig))).astype(jnp.bfloat16)
    d_up = (d_act * gate_swish).astype(jnp.bfloat16)
    dw_gate = jnp.dot(h_norm.T, d_gate, preferred_element_type=jnp.float32)
    dw_up = jnp.dot(h_norm.T, d_up, preferred_element_type=jnp.float32)
    d_hnorm = (jnp.dot(d_gate, w_gate.T, preferred_element_type=jnp.float32)
               + jnp.dot(d_up, w_up.T, preferred_element_type=jnp.float32))
    d_gain = jnp.sum(d_hnorm * x_hat, axis=0)
    d_xhat = d_hnorm * ln_gain
    dx_ln = inv_std * (d_xhat - jnp.mean(d_xhat, axis=1, keepdims=True)
                       - x_hat * jnp.mean(d_xhat * x_hat, axis=1, keepdims=True))
    dx_tok = (dy_tok.astype(jnp.float32) + dx_ln).astype(jnp.bfloat16)
    return (y_tok, dx_tok, dw_gate, dw_up, dw_down, d_gain)
```

```python
import jax
import jax.numpy as jnp
from jax import lax
from jax.sharding import PartitionSpec as P

LN_EPS = 1e-6
CHIP = [[0, 1], [2, 3]]


def contract_rows(left_op, right_op):
    return lax.dot_general(left_op, right_op, (((0,), (0,)), ((), ())), preferred_element_type=jnp.float32)


def contract_cols(left_op, right_op):
    return lax.dot_general(left_op, right_op, (((1,), (1,)), ((), ())), preferred_element_type=jnp.float32)


def solution(mesh):
    tx_size = mesh.shape["tx"]

    def local_step(x_blk, dy_blk, gain_blk, w_gate_blk, w_up_blk, w_down_blk):
        rows, cols = x_blk.shape
        d_model = cols * tx_size
        f_loc = w_gate_blk.shape[1]
        half = f_loc // 2
        core = lax.rem(lax.axis_index("tx"), 2)
        tx = lax.axis_index("tx")

        def pick(w):
            return lax.dynamic_slice_in_dim(w, core * half, half, axis=1)

        w_gate_all = pick(lax.all_gather(w_gate_blk, "tx", axis=0, tiled=True))
        w_up_all = pick(lax.all_gather(w_up_blk, "tx", axis=0, tiled=True))
        w_down_all = lax.dynamic_slice_in_dim(lax.all_gather(w_down_blk, "tx", axis=1, tiled=True), core * half, half, 0)
        gain_all = lax.all_gather(gain_blk, "tx", axis=0, tiled=True)
        x_row = lax.all_gather(x_blk, "tx", axis=1, tiled=True)
        x_all = lax.all_gather(x_row, "ty", axis=0, tiled=True)
        dy_row = lax.all_gather(dy_blk, "tx", axis=1, tiled=True)
        dy_all = lax.all_gather(dy_row, "ty", axis=0, tiled=True)

        xf = x_all.astype(jnp.float32)
        mean_x = jnp.sum(xf, axis=1, keepdims=True) / d_model
        mean_s = jnp.sum(xf * xf, axis=1, keepdims=True) / d_model
        inv_all = lax.rsqrt(mean_s - mean_x * mean_x + LN_EPS)
        h_all = (gain_all * ((xf - mean_x) * inv_all)).astype(jnp.bfloat16)
        my_row = lax.axis_index("ty") * rows
        mu = lax.dynamic_slice_in_dim(mean_x, my_row, rows, 0)
        inv_std = lax.dynamic_slice_in_dim(inv_all, my_row, rows, 0)
        x_float = x_blk.astype(jnp.float32)
        x_hat = (x_float - mu) * inv_std

        u = jnp.dot(h_all, w_gate_all, preferred_element_type=jnp.float32)
        v = jnp.dot(h_all, w_up_all, preferred_element_type=jnp.float32)
        sig = jax.nn.sigmoid(u)
        swish = u * sig
        act = (swish * v).astype(jnp.bfloat16)
        d_act = contract_cols(dy_all, w_down_all)
        d_gate = (d_act * v * sig * (1.0 + u * (1.0 - sig))).astype(jnp.bfloat16)
        d_up = (d_act * swish).astype(jnp.bfloat16)

        def pair(a):
            return lax.all_gather(a, "tx", axis=1, tiled=True, axis_index_groups=CHIP)

        act_all, d_gate_all, d_up_all = pair(act), pair(d_gate), pair(d_up)
        mlp_out = lax.psum_scatter(jnp.dot(act_all, w_down_blk, preferred_element_type=jnp.float32),
                                   "ty", scatter_dimension=0, tiled=True)
        y_blk = (x_float + mlp_out).astype(jnp.bfloat16)
        d_hnorm = lax.psum_scatter(contract_cols(d_gate_all, w_gate_blk) + contract_cols(d_up_all, w_up_blk),
                                   "ty", scatter_dimension=0, tiled=True)
        h_my = lax.dynamic_slice_in_dim(h_all, tx * cols, cols, 1)
        dy_my = lax.dynamic_slice_in_dim(dy_all, tx * cols, cols, 1)
        dw_down_blk = contract_rows(act_all, dy_my)
        dw_gate_blk = contract_rows(h_my, d_gate_all)
        dw_up_blk = contract_rows(h_my, d_up_all)
        e = d_hnorm * gain_blk
        bwd_stats = lax.psum(jnp.stack([jnp.sum(e, axis=1), jnp.sum(e * x_hat, axis=1)]), "tx") / d_model
        dx_ln = inv_std * (e - bwd_stats[0][:, None] - x_hat * bwd_stats[1][:, None])
        dx_blk = (dy_blk.astype(jnp.float32) + dx_ln).astype(jnp.bfloat16)
        d_gain_blk = lax.psum(jnp.sum(d_hnorm * x_hat, axis=0), "ty")
        return (y_blk, dx_blk, dw_gate_blk, dw_up_blk, dw_down_blk, d_gain_blk)

    return jax.shard_map(
        local_step, mesh=mesh,
        in_specs=(P("ty", "tx"), P("ty", "tx"), P("tx"), P("tx", "ty"), P("tx", "ty"), P("ty", "tx")),
        out_specs=(P("ty", "tx"), P("ty", "tx"), P("tx", "ty"), P("tx", "ty"), P("ty", "tx"), P("tx")),
        check_vma=False)
```

```python
import jax
import jax.numpy as jnp
from jax import lax
from jax.experimental import pallas as pl
from jax.experimental.pallas import tpu as pltpu
from jax.sharding import PartitionSpec as P

LN_EPS = 1e-6
MESH = pl.DeviceIdType.MESH
BF16 = jnp.bfloat16
F32 = jnp.float32
STEPS = 8
ROWS = 128
TOK = 4 * ROWS
DQ = 512
DM = 4 * DQ
FB = 2048
FH = FB // 2
NT = (((1,), (1,)), ((), ()))
X, YA, YB, YBF, ZA, ZB, ZAF, C0, C1 = range(9)


def kernel(x_ref, dy_ref, g_ref, wg_ref, wu_ref, wd_ref,
           y_ref, dx_ref, dw1_ref, dw3_ref, dw2_ref, dg_ref,
           xg, dyg, hg, ug, vg, ag, dug, dvg, rcv1, rcv2,
           w1g, w3g, w2g, w1o, w3o, w2o, acc1, acc3, acc2, b0, b1, dyb, ab, ub, vb,
           hq, hqt, dyq, dyqt, xown, dyown, part, r1, r2, gfull, gsrc, st, stall, dhs, yst,
           pst, pstr, dgs, dgr,
           gs, gr, ws, wr, ggs, ggr, cs, cr, rss, rsr, ss, sr, dgss, dgsr, loc, hst, ust, qst, pstm, ast, hld, uld, ald,
           dld, xld, rld, yld, wst):
    ty = lax.axis_index("ty")
    tx = lax.axis_index("tx")
    y = ty % 2
    z = ty // 2
    c = tx % 2
    tx2 = (tx + 2) % 4
    ty_y = ty + 1 - 2 * y
    ty_z = (ty + 2) % 4
    XP = (ty, tx2)
    CP = (ty, tx + 1 - 2 * c)
    XC = (ty, tx2 + 1 - 2 * c)
    YP = (ty_y, tx)
    ZP = (ty_z, tx)
    YZ = (ty_z + 1 - 2 * y, tx)

    def rc(src, dst, s, r, dev):
        return pltpu.make_async_remote_copy(src_ref=src, dst_ref=dst, send_sem=s, recv_sem=r,
                                            device_id=dev, device_id_type=MESH)

    def lc(src, dst, s):
        return pltpu.make_async_copy(src, dst, s)

    def row(j):
        return pl.ds(pl.multiple_of(j * ROWS, ROWS), ROWS)

    def qcol(q):
        return pl.ds(pl.multiple_of(q * DQ, DQ), DQ)

    def hcol(h):
        return pl.ds(pl.multiple_of(h * FH, FH), FH)

    def gcopy(arr, kind, s):
        own, buf = ((x_ref, xg), (dy_ref, dyg))[arr]
        a, b = gs.at[arr, kind, s], gr.at[arr, kind, s]
        mine = buf.at[tx, s, row(ty)]
        other = buf.at[tx2, s, row(ty)]
        if kind == X:
            return rc(own.at[s], mine, a, b, XP)
        if kind == YA:
            return rc(own.at[s], mine, a, b, YP)
        if kind == ZA:
            return rc(own.at[s], mine, a, b, ZP)
        if kind == YB:
            return rc(other, other, a, b, YP)
        if kind == ZB:
            return rc(other, other, a, b, ZP)
        if kind == ZAF:
            blk = buf.at[tx, s, row(ty_y)]
            return rc(blk, blk, a, b, ZP)
        if kind == YBF:
            blk = buf.at[tx2, s, row(ty_z)]
            return rc(blk, blk, a, b, YP)
        blk = buf.at[tx if kind == C0 else tx2, s]
        return rc(blk, blk, a, b, CP)

    def loop(n, f):
        def body(s, carry):
            f(s)
            return carry
        lax.fori_loop(0, n, body, 0)

    def wcopy(w, k):
        dev, h = ((XP, c), (XC, 1 - c), (CP, 1 - c))[k]
        a, b = ws.at[w, k], wr.at[w, k]
        if w < 2:
            return rc((wg_ref, wu_ref)[w].at[:, hcol(h)], (w1g, w3g)[w].at[qcol(tx), :], a, b, dev)
        return rc(wd_ref.at[hcol(h), :], w2g.at[:, qcol(tx)], a, b, dev)

    def gaincopy(k):
        return rc(gsrc, gfull.at[:, qcol(tx)], ggs.at[k], ggr.at[k], (XP, XC, CP)[k])

    gsrc[...] = jnp.broadcast_to(g_ref[...], (8, DQ))
    barrier = pltpu.get_barrier_semaphore()
    for dev in (XP, CP, XC, YP, ZP, YZ):
        pl.semaphore_signal(barrier, inc=1, device_id=dev, device_id_type=MESH)
    own_in = [lc(x_ref, xown, loc.at[0]), lc(dy_ref, dyown, loc.at[1])]
    w_in = [lc(wg_ref, w1o, loc.at[2]), lc(wu_ref, w3o, loc.at[3]), lc(wd_ref, w2o, loc.at[4]),
            lc(wg_ref.at[:, hcol(c)], w1g.at[qcol(tx), :], loc.at[5]),
            lc(wu_ref.at[:, hcol(c)], w3g.at[qcol(tx), :], loc.at[6]),
            lc(wd_ref.at[hcol(c), :], w2g.at[:, qcol(tx)], loc.at[7])]
    for d in own_in:
        d.start()
    pl.semaphore_wait(barrier, 6)

    for k in range(3):
        gaincopy(k).start()
    loop(STEPS, lambda s: gcopy(0, X, s).start())

    def send_a(s):
        gcopy(0, YA, s).start()
        gcopy(0, ZA, s).start()
    loop(STEPS, send_a)
    for w in range(2):
        for k in range(3):
            wcopy(w, k).start()
    loop(STEPS, lambda s: gcopy(1, X, s).start())
    for k in range(3):
        wcopy(2, k).start()
    for d in w_in:
        d.start()
    for d in own_in:
        d.wait()
    own_out = [lc(xown, xg.at[tx, :, row(ty)], loc.at[0]), lc(dyown, dyg.at[tx, :, row(ty)], loc.at[1])]
    for d in own_out:
        d.start()
    gfull[:, qcol(tx)] = gsrc[...]

    def l1(arr, s):
        gcopy(arr, X, s).wait_recv()
        gcopy(arr, YB, s).start()
        gcopy(arr, ZB, s).start()

    def l1f(arr, s):
        gcopy(arr, YA, s).wait_recv()
        gcopy(arr, ZAF, s).start()

    def l2(arr, s):
        gcopy(arr, ZB, s).wait_recv()
        gcopy(arr, YBF, s).start()

    def l3(arr, s):
        gcopy(arr, ZA, s).wait_recv()
        gcopy(arr, ZAF, s).wait_recv()
        gcopy(arr, C0, s).start()
        gcopy(arr, YB, s).wait_recv()
        gcopy(arr, YBF, s).wait_recv()
        gcopy(arr, C1, s).start()

    def first(s):
        l1(0, s)
        l1f(0, s)
    loop(STEPS, first)
    loop(STEPS, lambda s: l2(0, s))

    def send_dya(s):
        gcopy(1, YA, s).start()
        gcopy(1, ZA, s).start()
    loop(STEPS, send_dya)
    for d in own_out:
        d.wait()
    for d in w_in:
        d.wait()
    for k in range(3):
        gaincopy(k).wait_recv()
    loop(STEPS, lambda s: l3(0, s))

    def block_loads(arr, s, dst, sem):
        buf = (xg, dyg)[arr]
        return [lc(buf.at[q, s], dst.at[:, q * DQ:(q + 1) * DQ], sem.at[q]) for q in range(4)]

    def wait_block(arr, s):
        gcopy(arr, C0, s).wait_recv()
        gcopy(arr, C1, s).wait_recv()

    xs, hb = b1.at[0], b1.at[1]

    def h_store(s):
        return lc(hb, hg.at[s], hst.at[0])

    def u_store(s):
        return lc(acc2.at[:, hcol(s % 2)], ug.at[s], ust.at[s % 2])

    wait_block(0, 0)
    for d in block_loads(0, 0, xs, xld):
        d.start()
    for k in range(3):
        wcopy(0, k).wait_recv()

    def pass1(s):
        for d in block_loads(0, s, xs, xld):
            d.wait()

        @pl.when(s >= 1)
        def _():
            h_store(s - 1).wait()

        def chunk(i):
            rr = pl.ds(pl.multiple_of(i * 64, 64), 64)
            xf = xs[rr, :].astype(F32)
            mu = jnp.sum(xf, axis=1, keepdims=True) * (1.0 / DM)
            sq = jnp.sum(xf * xf, axis=1, keepdims=True) * (1.0 / DM)
            inv = lax.rsqrt(sq - mu * mu + LN_EPS)
            hb[rr, :] = (gfull[0:1, :] * ((xf - mu) * inv)).astype(BF16)
            lane = lax.broadcasted_iota(jnp.int32, (64, 128), 1)
            stall[rr, :] = jnp.where(lane == 0, mu, inv)
        loop(TOK // 64, chunk)
        st[s] = stall[row(ty), :]
        h_store(s).start()

        @pl.when(s < STEPS - 1)
        def _():
            wait_block(0, s + 1)
            for d in block_loads(0, s + 1, xs, xld):
                d.start()

        @pl.when(s >= 2)
        def _():
            u_store(s - 2).wait()
        acc2[:, hcol(s % 2)] = jnp.dot(hb[...], w1g[...], preferred_element_type=F32)
        u_store(s).start()
        l1f(1, s)
    loop(STEPS, pass1)
    h_store(STEPS - 1).wait()
    u_store(STEPS - 2).wait()
    u_store(STEPS - 1).wait()

    def rs_copy(kind, n):
        slot = n % 3
        a, b = rss.at[kind, n], rsr.at[kind, n]
        if kind == 0:
            return rc(part.at[slot, 0, 1 - y], rcv1.at[n, 0], a, b, YP)
        if kind == 1:
            return rc(part.at[slot, 1, 1 - z], rcv1.at[n, 1], a, b, ZP)
        if kind == 2:
            return rc(part.at[slot, 0, y, 1 - z], rcv2.at[n, 0], a, b, ZP)
        return rc(part.at[slot, 1, z, 1 - y], rcv2.at[n, 1], a, b, YP)

    def rs_put(n, val):
        slot = n % 3
        for j in range(4):
            part[slot, 0, j % 2, j // 2] = val[j * ROWS:(j + 1) * ROWS, 0:256]
            part[slot, 1, j // 2, j % 2] = val[j * ROWS:(j + 1) * ROWS, 256:512]

    def rs_first(n):
        rs_copy(0, n).start()
        rs_copy(1, n).start()

    def rs_loads(K):
        @pl.when((K >= 2) & (K <= 17))
        def _():
            rs_copy(0, K - 2).wait_recv()
            rs_copy(1, K - 2).wait_recv()
            lc(rcv1.at[K - 2], r1, rld.at[0]).start()

        @pl.when((K >= 3) & (K <= 18))
        def _():
            rs_copy(2, K - 3).wait_recv()
            rs_copy(3, K - 3).wait_recv()
            lc(rcv2.at[K - 3], r2, rld.at[1]).start()

    def y_store(n):
        return lc(yst.at[n % 2], y_ref.at[n], yld.at[n % 2])

    def rs_proc(K):
        @pl.when((K >= 2) & (K <= 17))
        def _():
            n = K - 2
            slot = n % 3
            lc(rcv1.at[n], r1, rld.at[0]).wait()
            for k in range(2):
                part[slot, 0, y, k] += r1[0, k]
                part[slot, 1, z, k] += r1[1, k]
            rs_copy(2, n).start()
            rs_copy(3, n).start()

        @pl.when((K >= 3) & (K <= 18))
        def _():
            n = K - 3
            slot = n % 3
            lc(rcv2.at[n], r2, rld.at[1]).wait()
            for k in range(4):
                rs_copy(k, n).wait_send()

            @pl.when(n < 8)
            def _():
                @pl.when(n >= 2)
                def _():
                    y_store(n - 2).wait()
                yst[n % 2, :, 0:256] = (xown[n, :, 0:256].astype(F32) + (part[slot, 0, y, z] + r2[0])).astype(BF16)
                yst[n % 2, :, 256:512] = (xown[n, :, 256:512].astype(F32) + (part[slot, 1, z, y] + r2[1])).astype(BF16)
                y_store(n).start()

            @pl.when(n >= 8)
            def _():
                s = n - 8
                dhs[s, :, 0:256] = part[slot, 0, y, z] + r2[0]
                dhs[s, :, 256:512] = part[slot, 1, z, y] + r2[1]
                dh = dhs[s]
                xh = (xown[s].astype(F32) - st[s, :, 0:1]) * st[s, :, 1:2]
                ev = dh * gsrc[0:1, :]
                dgs[...] += jnp.sum((dh * xh).reshape(ROWS // 8, 8, DQ), axis=0)
                s1 = jnp.sum(ev, axis=1, keepdims=True)
                s2 = jnp.sum(ev * xh, axis=1, keepdims=True)
                lane = lax.broadcasted_iota(jnp.int32, (ROWS, 128), 1)
                mat = jnp.where(lane == 0, s1, jnp.where(lane == 1, s2, 0.0))
                pst[s] = mat.T[0:8, :]

    def h_load(s):
        return lc(hg.at[s], b1.at[s % 2], hld.at[s % 2])

    def u_load(s):
        return lc(ug.at[s], acc1.at[:, hcol(s % 2)], uld.at[s % 2])

    def q_store(s):
        return lc(acc1.at[:, hcol(s % 2)], ug.at[s], qst.at[s % 2])

    def p_store(s):
        return lc(acc3.at[:, hcol(s % 2)], vg.at[s], pstm.at[s % 2])

    def a_store(s):
        return lc(b0.at[s % 2, :, hcol(c)], ag.at[s, :, hcol(c)], ast.at[s % 2])

    def a_send(s):
        return rc(b0.at[s % 2, :, hcol(c)], ag.at[s, :, hcol(c)], cs.at[0, s], cr.at[0, s], CP)

    def a_load(s):
        return lc(ag.at[s, :, hcol(1 - c)], b0.at[s % 2, :, hcol(1 - c)], ald.at[0])

    def make_m(n):
        a_load(n).wait()
        rs_put(n, jnp.dot(b0[n % 2], w2o[...], preferred_element_type=F32))
        rs_first(n)

    h_load(0).start()
    u_load(0).start()
    dgs[...] = jnp.zeros_like(dgs)
    for k in range(3):
        wcopy(1, k).wait_recv()

    def pass2(K):
        s = K
        l1(1, s)

        @pl.when(K >= 2)
        def _():
            l2(1, K - 2)

        @pl.when(K >= 4)
        def _():
            l3(1, K - 4)

        @pl.when(K >= 1)
        def _():
            a_send(K - 1).wait_recv()
            a_load(K - 1).start()
            q_store(K - 1).wait()
        h_load(s).wait()
        u_load(s).wait()

        @pl.when(s < STEPS - 1)
        def _():
            h_load(s + 1).start()
            u_load(s + 1).start()

        @pl.when(s >= 2)
        def _():
            p_store(s - 2).wait()
            a_store(s - 2).wait()
            a_send(s - 2).wait_send()
        for k in range(2):
            cc = pl.ds(pl.multiple_of((s % 2) * FH + k * 512, 512), 512)
            v = jnp.dot(b1[s % 2], w3g[:, k * 512:(k + 1) * 512], preferred_element_type=F32)
            u = acc1[:, cc]
            sig = jax.nn.sigmoid(u)
            q = u * sig
            b0[s % 2, :, pl.ds(pl.multiple_of(c * FH + k * 512, 512), 512)] = (q * v).astype(BF16)
            acc3[:, cc] = v * sig * (1.0 + u * (1.0 - sig))
            acc1[:, cc] = q
        a_send(s).start()
        a_store(s).start()
        q_store(s).start()
        p_store(s).start()
        rs_loads(K)

        @pl.when(K >= 1)
        def _():
            make_m(K - 1)
        rs_proc(K)
    loop(STEPS, pass2)
    l2(1, STEPS - 2)
    l2(1, STEPS - 1)
    q_store(STEPS - 1).wait()
    for s in (STEPS - 2, STEPS - 1):
        p_store(s).wait()
        a_store(s).wait()

    def qp_loads(s):
        return [lc(ug.at[s], ub, dld.at[0]), lc(vg.at[s], vb, dld.at[1])]

    def d_send(w, s):
        src, dst = ((b0, dug), (b1, dvg))[w]
        return rc(src.at[s % 2, :, hcol(c)], dst.at[s], cs.at[1 + w, s], cr.at[1 + w, s], CP)

    def d_loads(s):
        return [lc(dug.at[s], b0.at[s % 2, :, hcol(1 - c)], ald.at[0]),
                lc(dvg.at[s], b1.at[s % 2, :, hcol(1 - c)], ald.at[1])]

    def w_loads(s):
        return [lc(ag.at[s], ab, ald.at[2]), lc(hg.at[s, :, qcol(tx)], hq, ald.at[3]), lc(dyg.at[tx, s], dyq, ald.at[4])]

    def next_loads(s):
        wait_block(1, s)
        for d in block_loads(1, s, dyb, xld) + qp_loads(s):
            d.start()

    a_send(STEPS - 1).wait_recv()
    a_load(STEPS - 1).start()
    for k in range(3):
        wcopy(2, k).wait_recv()
    next_loads(0)

    def st_copy(k, s):
        return rc(pst.at[s], pstr.at[k, s], ss.at[k, s], sr.at[k, s], (XP, XC, CP)[k])

    def pass3(i):
        K = i + 8
        s = i

        @pl.when(s < 4)
        def _():
            l3(1, s + 4)

        @pl.when((K >= 9) & (K <= 16))
        def _():
            d_send(0, K - 9).wait_recv()
            d_send(1, K - 9).wait_recv()
            for d in d_loads(K - 9) + w_loads(K - 9):
                d.start()

        @pl.when(s < STEPS)
        def _():
            for d in block_loads(1, s, dyb, xld) + qp_loads(s):
                d.wait()

            @pl.when(s < 2)
            def _():
                a_send(STEPS - 2 + s).wait_send()

            @pl.when(s >= 2)
            def _():
                d_send(0, s - 2).wait_send()
                d_send(1, s - 2).wait_send()
            for k in range(2):
                cc = pl.ds(pl.multiple_of(c * FH + k * 512, 512), 512)
                kk = slice(k * 512, (k + 1) * 512)
                da = lax.dot_general(dyb[...], w2g[kk, :], NT, preferred_element_type=F32)
                b0[s % 2, :, cc] = (da * vb[:, kk]).astype(BF16)
                b1[s % 2, :, cc] = (da * ub[:, kk]).astype(BF16)
            d_send(0, s).start()
            d_send(1, s).start()

            @pl.when(s < STEPS - 1)
            def _():
                next_loads(s + 1)
        rs_loads(K)

        @pl.when(K == 8)
        def _():
            make_m(STEPS - 1)
            for acc in (acc1, acc3, acc2):
                def zero(j):
                    acc[pl.ds(pl.multiple_of(j * 16, 16), 16), :] = jnp.zeros((16, FB), F32)
                loop(DQ // 16, zero)

        @pl.when((K >= 9) & (K <= 16))
        def _():
            n = K - 9
            for d in d_loads(n):
                d.wait()
            rs_put(8 + n, lax.dot_general(b0[n % 2], w1o[...], NT, preferred_element_type=F32)
                   + lax.dot_general(b1[n % 2], w3o[...], NT, preferred_element_type=F32))
            rs_first(8 + n)

        @pl.when(K >= 12)
        def _():
            for k in range(3):
                st_copy(k, K - 12).start()
        rs_proc(K)

        @pl.when((K >= 9) & (K <= 16))
        def _():
            n = K - 9
            for d in w_loads(n):
                d.wait()
            hqt[...] = hq[...].T
            dyqt[...] = dyq[...].T
            acc1[...] += jnp.dot(hqt[...], b0[n % 2], preferred_element_type=F32)
            acc3[...] += jnp.dot(hqt[...], b1[n % 2], preferred_element_type=F32)
            acc2[...] += jnp.dot(dyqt[...], ab[...], preferred_element_type=F32)

        @pl.when(K == 16)
        def _():
            for k, (acc, out) in enumerate(((acc1, dw1_ref), (acc3, dw3_ref), (acc2, dw2_ref))):
                lc(acc, out, wst.at[k]).start()
    loop(STEPS + 3, pass3)

    for k in range(3):
        st_copy(k, STEPS - 1).start()

    def dg_copy(k):
        return rc(dgs, dgr.at[k], dgss.at[k], dgsr.at[k], (YP, ZP, YZ)[k])
    for k in range(3):
        dg_copy(k).start()

    def dx_step(s):
        for k in range(3):
            st_copy(k, s).wait_recv()
        tot = pst[s] + pstr[0, s] + pstr[1, s] + pstr[2, s]
        mat = jnp.concatenate([tot, jnp.zeros((120, 128), F32)], axis=0).T
        m1 = mat[:, 0:1] * (1.0 / DM)
        m2 = mat[:, 1:2] * (1.0 / DM)
        inv = st[s, :, 1:2]
        xh = (xown[s].astype(F32) - st[s, :, 0:1]) * inv
        ev = dhs[s] * gsrc[0:1, :]
        dyown[s] = (dyown[s].astype(F32) + inv * (ev - m1 - xh * m2)).astype(BF16)
    loop(STEPS, dx_step)
    dx_out = lc(dyown, dx_ref, loc.at[0])
    dx_out.start()
    for k in range(3):
        dg_copy(k).wait_recv()
    tot = dgs[...] + dgr[0] + dgr[1] + dgr[2]
    dg_ref[...] = jnp.broadcast_to(jnp.sum(tot, axis=0, keepdims=True), (8, DQ))

    for k, (acc, out) in enumerate(((acc1, dw1_ref), (acc3, dw3_ref), (acc2, dw2_ref))):
        lc(acc, out, wst.at[k]).wait()
    y_store(STEPS - 2).wait()
    y_store(STEPS - 1).wait()
    for s in (STEPS - 2, STEPS - 1):
        d_send(0, s).wait_send()
        d_send(1, s).wait_send()

    def drain(s):
        for arr in range(2):
            for kind in range(9):
                gcopy(arr, kind, s).wait_send()
        for k in range(3):
            st_copy(k, s).wait_send()
    loop(STEPS, drain)
    for k in range(3):
        gaincopy(k).wait_send()
        dg_copy(k).wait_send()
        for w in range(3):
            wcopy(w, k).wait_send()
    dx_out.wait()


def solution(mesh):
    any_spec = pl.BlockSpec(memory_space=pl.ANY)
    vmem_spec = pl.BlockSpec(memory_space=pltpu.VMEM)
    sd = jax.ShapeDtypeStruct
    dma = pltpu.SemaphoreType.DMA

    def local_step(x_blk, dy_blk, gain_blk, w_gate_blk, w_up_blk, w_down_blk):
        outs = pl.pallas_call(
            kernel,
            out_shape=[
                sd((STEPS, ROWS, DQ), BF16), sd((STEPS, ROWS, DQ), BF16),
                sd((DQ, FB), F32), sd((DQ, FB), F32), sd((DQ, FB), F32), sd((8, DQ), F32),
                sd((4, STEPS, TOK, DQ), BF16), sd((4, STEPS, TOK, DQ), BF16),
                sd((STEPS, TOK, DM), BF16), sd((STEPS, TOK, FH), F32), sd((STEPS, TOK, FH), F32),
                sd((STEPS, TOK, FB), BF16), sd((STEPS, TOK, FH), BF16), sd((STEPS, TOK, FH), BF16),
                sd((2 * STEPS, 2, 2, ROWS, 256), F32), sd((2 * STEPS, 2, ROWS, 256), F32),
            ],
            in_specs=[any_spec, any_spec, vmem_spec, any_spec, any_spec, any_spec],
            out_specs=[any_spec] * 5 + [vmem_spec] + [any_spec] * 10,
            scratch_shapes=[
                pltpu.VMEM((DM, FH), BF16), pltpu.VMEM((DM, FH), BF16), pltpu.VMEM((FH, DM), BF16),
                pltpu.VMEM((DQ, FB), BF16), pltpu.VMEM((DQ, FB), BF16), pltpu.VMEM((FB, DQ), BF16),
                pltpu.VMEM((DQ, FB), F32), pltpu.VMEM((DQ, FB), F32), pltpu.VMEM((DQ, FB), F32),
                pltpu.VMEM((2, TOK, FB), BF16), pltpu.VMEM((2, TOK, FB), BF16),
                pltpu.VMEM((TOK, DM), BF16), pltpu.VMEM((TOK, FB), BF16),
                pltpu.VMEM((TOK, FH), F32), pltpu.VMEM((TOK, FH), F32),
                pltpu.VMEM((TOK, DQ), BF16), pltpu.VMEM((DQ, TOK), BF16),
                pltpu.VMEM((TOK, DQ), BF16), pltpu.VMEM((DQ, TOK), BF16),
                pltpu.VMEM((STEPS, ROWS, DQ), BF16), pltpu.VMEM((STEPS, ROWS, DQ), BF16),
                pltpu.VMEM((3, 2, 2, 2, ROWS, 256), F32),
                pltpu.VMEM((2, 2, ROWS, 256), F32), pltpu.VMEM((2, ROWS, 256), F32),
                pltpu.VMEM((8, DM), F32), pltpu.VMEM((8, DQ), F32),
                pltpu.VMEM((STEPS, ROWS, 128), F32), pltpu.VMEM((TOK, 128), F32),
                pltpu.VMEM((STEPS, ROWS, DQ), F32), pltpu.VMEM((2, ROWS, DQ), BF16),
                pltpu.VMEM((STEPS, 8, 128), F32), pltpu.VMEM((3, STEPS, 8, 128), F32),
                pltpu.VMEM((8, DQ), F32), pltpu.VMEM((3, 8, DQ), F32),
                dma((2, 9, STEPS)), dma((2, 9, STEPS)), dma((3, 3)), dma((3, 3)), dma((3,)), dma((3,)),
                dma((3, STEPS)), dma((3, STEPS)), dma((4, 2 * STEPS)), dma((4, 2 * STEPS)),
                dma((3, STEPS)), dma((3, STEPS)), dma((3,)), dma((3,)),
                dma((8,)), dma((1,)), dma((2,)), dma((2,)), dma((2,)), dma((2,)), dma((2,)), dma((2,)), dma((5,)),
                dma((2,)), dma((4,)), dma((2,)), dma((2,)), dma((3,)),
            ],
            compiler_params=pltpu.CompilerParams(collective_id=0, has_side_effects=True,
                                                 vmem_limit_bytes=67043328),
        )(x_blk.reshape(STEPS, ROWS, DQ), dy_blk.reshape(STEPS, ROWS, DQ), gain_blk.reshape(1, DQ),
          w_gate_blk, w_up_blk, w_down_blk)
        y_blk, dx_blk, dw1, dw3, dw2t, dg = outs[:6]
        return (y_blk.reshape(STEPS * ROWS, DQ), dx_blk.reshape(STEPS * ROWS, DQ), dw1, dw3, dw2t.T, dg[0])

    return jax.shard_map(
        local_step, mesh=mesh,
        in_specs=(P("ty", "tx"), P("ty", "tx"), P("tx"), P("tx", "ty"), P("tx", "ty"), P("ty", "tx")),
        out_specs=(P("ty", "tx"), P("ty", "tx"), P("tx", "ty"), P("tx", "ty"), P("ty", "tx"), P("tx")),
        check_vma=False)
```

```python
import jax
import jax.numpy as jnp
from jax import lax
from jax.experimental import pallas as pl
from jax.experimental.pallas import tpu as pltpu
from jax.sharding import PartitionSpec as P

LN_EPS = 1e-6
MESH = pl.DeviceIdType.MESH
BF16 = jnp.bfloat16
F32 = jnp.float32
STEPS = 8
ROWS = 128
TOK = 4 * ROWS
DQ = 512
DM = 4 * DQ
FB = 2048
FH = FB // 2
NT = (((1,), (1,)), ((), ()))
INV_DM = 1.0 / DM
PAIR, TRIO = range(2), range(3)
X, YA, YB, YBF, ZA, ZB, ZAF, C0, C1, YAF, XR = range(11)
RECV = [0, 1, 2, 2, 3, 4, 3, 5, 5, 1, 0]
DIRECT = 2
N_RS = 2 * STEPS
N_YAF = (STEPS - DIRECT) // 2


def alt(n):
    return n % 2


def kernel(x_ref, dy_ref, g_ref, wg_ref, wu_ref, wd_ref,
           y_ref, dx_ref, acc1, acc3, acc2, dg_ref,
           xg, dyg, hg, ug, vg,
           w1g, w3g, w2g, w2o, b0, b1, dyb, ub, vb,
           hq, hqt, xown, dyown, part, r1, r2, gfull, gsrc, st, stall, dhs,
           pst, pstr, dgs, dgr,
           gs, gr, ws, wr, ggs, ggr, cs, cr, rss, rsr, ss, sr, dgss, dgsr, loc, hst, ust, qst, pstm, hld, uld, ald,
           dld, xld, credit):
    ty = lax.axis_index("ty")
    tx = lax.axis_index("tx")
    y = ty % 2
    z = ty // 2
    c = tx % 2
    tx2 = (tx + 2) % 4
    ty_y = ty + 1 - 2 * y
    ty_z = (ty + 2) % 4
    XP = (ty, tx2)
    CP = (ty, tx + 1 - 2 * c)
    XC = (ty, tx2 + 1 - 2 * c)
    YP = (ty_y, tx)
    ZP = (ty_z, tx)
    YZ = (ty_z + 1 - 2 * y, tx)

    def rc(src, dst, s, r, dev):
        return pltpu.make_async_remote_copy(src_ref=src, dst_ref=dst, send_sem=s, recv_sem=r,
                                            device_id=dev, device_id_type=MESH)

    def lc(src, dst, s):
        return pltpu.make_async_copy(src, dst, s)

    def row(j):
        return pl.ds(pl.multiple_of(j * ROWS, ROWS), ROWS)

    def qcol(q):
        return pl.ds(pl.multiple_of(q * DQ, DQ), DQ)

    def hcol(h):
        return pl.ds(pl.multiple_of(h * FH, FH), FH)

    def gcopy(arr, kind, s):
        own, buf = ((x_ref, xg), (dy_ref, dyg))[arr]
        a, b = gs.at[arr, kind], gr.at[arr, RECV[kind], s]
        if kind in (X, YA, ZA):
            return rc(own.at[s], buf.at[tx, s, row(ty)], a, b, {X: XP, YA: YP, ZA: ZP}[kind])
        if kind in (YB, ZB):
            blk = buf.at[tx2, s, row(ty)]
            return rc(blk, blk, a, b, YP if kind == YB else ZP)
        if kind in (ZAF, YAF, YBF):
            blk = buf.at[tx2 if kind == YBF else tx, s, row(ty_y if kind == ZAF else ty_z)]
            return rc(blk, blk, a, b, ZP if kind == ZAF else YP)
        blk = buf.at[tx2 if kind == C1 else tx, s]
        return rc(blk, blk, a, b, XP if kind == XR else CP)

    def wait_bytes(ref, sem):
        lc(ref, ref, sem).wait()

    def pair_wait(arr, kind, s):
        wait_bytes(xg.at[0, s, 0:2 * ROWS], gr.at[arr, RECV[kind], s])

    def loop(n, f):
        def body(s, carry):
            f(s)
            return carry
        lax.fori_loop(0, n, body, 0)

    def wcopy(w, k):
        dev, h = ((XP, c), (XC, 1 - c), (CP, 1 - c))[k]
        a, b = ws.at[w, k], wr.at[w, k]
        if w < 2:
            return rc((wg_ref, wu_ref)[w].at[:, hcol(h)], (w1g, w3g)[w].at[qcol(tx), :], a, b, dev)
        return rc(wd_ref.at[hcol(h), :], w2g.at[:, qcol(tx)], a, b, dev)

    def gaincopy(k):
        return rc(gsrc, gfull.at[:, qcol(tx)], ggs.at[k], ggr.at[k], (XP, XC, CP)[k])

    gsrc[...] = jnp.broadcast_to(g_ref[...], (8, DQ))
    barrier = pltpu.get_barrier_semaphore()
    for dev in (XP, CP, XC, YP, ZP, YZ):
        pl.semaphore_signal(barrier, inc=1, device_id=dev, device_id_type=MESH)
    own_in = [lc(x_ref, xown, loc.at[0]), lc(dy_ref, dyown, loc.at[1])]
    w_in = [lc(wd_ref, w2o, loc.at[4]),
            lc(wg_ref.at[:, hcol(c)], w1g.at[qcol(tx), :], loc.at[5]),
            lc(wu_ref.at[:, hcol(c)], w3g.at[qcol(tx), :], loc.at[6]),
            lc(wd_ref.at[hcol(c), :], w2g.at[:, qcol(tx)], loc.at[7])]
    for d in own_in:
        d.start()
    with jax.named_scope("barrier"):
        pl.semaphore_wait(barrier, 6)

    for k in TRIO:
        gaincopy(k).start()
    loop(STEPS, lambda s: gcopy(0, X, s).start())

    def send_a(s):
        gcopy(0, YA, s).start()
        gcopy(0, ZA, s).start()
    loop(STEPS, send_a)
    for w in PAIR:
        for k in TRIO:
            wcopy(w, k).start()
    loop(DIRECT, lambda s: gcopy(1, X, s).start())
    for k in TRIO:
        wcopy(2, k).start()
    for d in w_in:
        d.start()
    for d in own_in:
        d.wait()
    own_out = [lc(xown, xg.at[tx, :, row(ty)], loc.at[0]), lc(dyown, dyg.at[tx, :, row(ty)], loc.at[1])]
    for d in own_out:
        d.start()
    gfull[:, qcol(tx)] = gsrc[...]

    def l1(arr, s):
        gcopy(arr, X, s).wait_recv()
        gcopy(arr, YB, s).start()
        gcopy(arr, ZB, s).start()

    def l1f(arr, s):
        gcopy(arr, YA, s).wait_recv()
        gcopy(arr, ZAF, s).start()

    def dy_forward(s):
        odd = (s >= DIRECT) & (alt(s) == 1)

        @pl.when(odd)
        def _():
            gcopy(1, ZA, s).wait_recv()
            gcopy(1, YAF, s).start()

        @pl.when(jnp.logical_not(odd))
        def _():
            gcopy(1, YA, s).wait_recv()
            gcopy(1, ZAF, s).start()

    def dy_quarter(s):
        odd = (s >= DIRECT) & (alt(s) == 1)

        @pl.when(odd)
        def _():
            pair_wait(1, YA, s)

        @pl.when(jnp.logical_not(odd))
        def _():
            pair_wait(1, ZA, s)
        gcopy(1, C0, s).start()

        @pl.when(s >= DIRECT)
        def _():
            gcopy(1, XR, s).start()

    def dy_rest(s):
        pair_wait(1, YB, s)
        gcopy(1, C1, s).start()

    def dy_cross(s):
        gcopy(1, XR, s).wait_recv()
        gcopy(1, C1, s).start()

    def l2(arr, s):
        gcopy(arr, ZB, s).wait_recv()
        gcopy(arr, YBF, s).start()

    def l3(arr, s):
        pair_wait(arr, ZA, s)
        gcopy(arr, C0, s).start()
        pair_wait(arr, YB, s)
        gcopy(arr, C1, s).start()

    def first(s):
        l1(0, s)
        l1f(0, s)
    with jax.named_scope("g_first"):
        loop(STEPS, first)
    with jax.named_scope("g_l2"):
        loop(STEPS, lambda s: l2(0, s))

    def send_dya(s):
        gcopy(1, YA, s).start()
        gcopy(1, ZA, s).start()
    loop(STEPS, send_dya)
    with jax.named_scope("g_local"):
        for d in own_out:
            d.wait()
        for d in w_in:
            d.wait()
        for k in TRIO:
            gaincopy(k).wait_recv()
    with jax.named_scope("g_l3"):
        loop(STEPS, lambda s: l3(0, s))

    def block_loads(arr, s, dst, sem):
        buf = (xg, dyg)[arr]
        return [lc(buf.at[q, s], dst.at[:, q * DQ:(q + 1) * DQ], sem.at[q]) for q in range(4)]

    def wait_block(arr, s):
        wait_bytes(xg.at[0:2, s], gr.at[arr, RECV[C0], s])

    xs, hb = b1.at[0], b1.at[1]

    def h_store(s):
        return lc(hb, hg.at[s], hst.at[0])

    def u_store(s):
        return lc(acc2.at[:, hcol(alt(s))], ug.at[s], ust.at[alt(s)])

    wait_block(0, 0)
    for d in block_loads(0, 0, xs, xld):
        d.start()
    with jax.named_scope("w1_wait"):
        for k in TRIO:
            wcopy(0, k).wait_recv()

    def pass1(s):
        with jax.named_scope("p1_xwait"):
            for d in block_loads(0, s, xs, xld):
                d.wait()

        @pl.when(s >= 1)
        def _():
            h_store(s - 1).wait()

        def chunk(i):
            rr = pl.ds(pl.multiple_of(i * 64, 64), 64)
            xf = xs[rr, :].astype(F32)
            mu = jnp.sum(xf, axis=1, keepdims=True) * INV_DM
            sq = jnp.sum(xf * xf, axis=1, keepdims=True) * INV_DM
            inv = lax.rsqrt(sq - mu * mu + LN_EPS)
            hb[rr, :] = (gfull[0:1, :] * ((xf - mu) * inv)).astype(BF16)
            lane = lax.broadcasted_iota(jnp.int32, (64, 128), 1)
            stall[rr, :] = jnp.where(lane == 0, mu, inv)
        with jax.named_scope("p1_ln"):
            loop(TOK // 64, chunk)
        st[s] = stall[row(ty), :]
        h_store(s).start()

        @pl.when(s < STEPS - 1)
        def _():
            wait_block(0, s + 1)
            for d in block_loads(0, s + 1, xs, xld):
                d.start()

        @pl.when(s >= 2)
        def _():
            u_store(s - 2).wait()
        with jax.named_scope("p1_dot"):
            acc2[:, hcol(alt(s))] = jnp.dot(hb[...], w1g[...], preferred_element_type=F32)
        u_store(s).start()
        with jax.named_scope("p1_fwd"):
            dy_forward(s)
    loop(STEPS, pass1)
    h_store(STEPS - 1).wait()
    u_store(STEPS - 2).wait()
    u_store(STEPS - 1).wait()

    def rs_copy(kind, n):
        slot = n % 3
        a, b = rss.at[kind, n % 4], rsr.at[kind, n % 4]
        if kind == 0:
            return rc(part.at[slot, 0, 1 - y], r1.at[n % 3, 0], a, b, YP)
        if kind == 1:
            return rc(part.at[slot, 1, 1 - z], r1.at[n % 3, 1], a, b, ZP)
        if kind == 2:
            return rc(part.at[slot, 0, y, 1 - z], r2.at[n % 3, 0], a, b, ZP)
        return rc(part.at[slot, 1, z, 1 - y], r2.at[n % 3, 1], a, b, YP)

    def rs_put(n, val):
        slot = n % 3
        for j in range(4):
            part[slot, 0, j % 2, j // 2] = val[j * ROWS:(j + 1) * ROWS, 0:256]
            part[slot, 1, j // 2, j % 2] = val[j * ROWS:(j + 1) * ROWS, 256:512]

    def rs_first(n):
        rs_copy(0, n).start()
        rs_copy(1, n).start()

    def rs_proc(K):
        @pl.when((K >= 2) & (K < N_RS + 2))
        def _():
            n = K - 2
            slot = n % 3
            for k in PAIR:
                rs_copy(k, n).wait_recv()
            for k in PAIR:
                part[slot, 0, y, k] += r1[slot, 0, k]
                part[slot, 1, z, k] += r1[slot, 1, k]
            rs_copy(2, n).start()
            rs_copy(3, n).start()

        @pl.when(K >= 3)
        def _():
            n = K - 3
            slot = n % 3
            for k in PAIR:
                rs_copy(2 + k, n).wait_recv()
            m0, m1 = r2[slot, 0], r2[slot, 1]
            for k in range(4):
                rs_copy(k, n).wait_send()

            @pl.when(n < 8)
            def _():
                y_ref[n, :, 0:256] = (xown[n, :, 0:256].astype(F32) + (part[slot, 0, y, z] + m0)).astype(BF16)
                y_ref[n, :, 256:512] = (xown[n, :, 256:512].astype(F32) + (part[slot, 1, z, y] + m1)).astype(BF16)

            @pl.when(n >= 8)
            def _():
                s = n - 8
                dhs[s % 4, :, 0:256] = part[slot, 0, y, z] + m0
                dhs[s % 4, :, 256:512] = part[slot, 1, z, y] + m1
                dh = dhs[s % 4]
                xh = (xown[s].astype(F32) - st[s, :, 0:1]) * st[s, :, 1:2]
                ev = dh * gsrc[0:1, :]
                dgs[...] += jnp.sum((dh * xh).reshape(ROWS // 8, 8, DQ), axis=0)
                s1 = jnp.sum(ev, axis=1, keepdims=True)
                s2 = jnp.sum(ev * xh, axis=1, keepdims=True)
                lane = lax.broadcasted_iota(jnp.int32, (ROWS, 128), 1)
                mat = jnp.where(lane == 0, s1, jnp.where(lane == 1, s2, 0.0))
                pst[s] = mat.T[0:8, :]

    def h_load(s):
        return lc(hg.at[s], b1.at[alt(s)], hld.at[alt(s)])

    def u_load(s):
        return lc(ug.at[s], acc1.at[:, hcol(alt(s))], uld.at[alt(s)])

    def q_store(s):
        return lc(acc1.at[:, hcol(alt(s))], ug.at[s], qst.at[alt(s)])

    def p_store(s):
        return lc(acc3.at[:, hcol(alt(s))], vg.at[s], pstm.at[alt(s)])

    def quart(k):
        return pl.ds(pl.multiple_of(c * FH + k * DQ, DQ), DQ)

    def swap(buf, s, k):
        blk = (b0, b1)[buf].at[alt(s), :, quart(k)]
        return rc(blk, blk, cs.at[buf, alt(s), k], cr.at[buf, alt(s), k], CP)

    def slot_free():
        pl.semaphore_signal(credit, inc=1, device_id=CP, device_id_type=MESH)

    def slot_wait():
        pl.semaphore_wait(credit, 1)

    def dyq_load(s):
        return lc(dyg.at[tx, s], hq, ald.at[1])

    def make_m(n):
        for k in PAIR:
            swap(0, n, k).wait_recv()
        rs_put(n, jnp.dot(b0[alt(n)], w2o[...], preferred_element_type=F32))
        rs_first(n)

    def add_dw2(n):
        dyq_load(n).wait()
        hqt[...] = hq[...].T
        acc2[...] += jnp.dot(hqt[...], b0[alt(n)], preferred_element_type=F32)
        slot_free()

    def zero(acc):
        def body(j):
            acc[pl.ds(pl.multiple_of(j * 16, 16), 16), :] = jnp.zeros((16, FB), F32)
        loop(DQ // 16, body)

    def qp_loads(s):
        return [lc(ug.at[s], ub, dld.at[0]), lc(vg.at[s], vb, dld.at[1])]

    def w_load(s):
        return lc(hg.at[s, :, qcol(tx)], hq, ald.at[0])

    def next_loads(s):
        wait_block(1, s)
        for d in block_loads(1, s, dyb, xld) + qp_loads(s):
            d.start()

    zero(acc2)
    h_load(0).start()
    u_load(0).start()
    dgs[...] = jnp.zeros_like(dgs)
    with jax.named_scope("w3_wait"):
        for k in TRIO:
            wcopy(1, k).wait_recv()

    own_w = [lc(w.at[:, hcol(h)], w1g.at[qcol(2 * k + h), :], loc.at[2 * k + h])
             for k, w in enumerate((wg_ref, wu_ref)) for h in PAIR]
    for d in own_w:
        d.start()

    def pass2(K):
        s = K
        with jax.named_scope("p2_comm"):
            dy_quarter(K)

            @pl.when((K >= 1) & (K <= DIRECT))
            def _():
                l1(1, K - 1)

            @pl.when((K >= 3) & (K <= 2 + DIRECT))
            def _():
                l2(1, K - 3)

            @pl.when((K >= 5) & (K <= 4 + DIRECT))
            def _():
                dy_rest(K - 5)

        @pl.when(K >= 1)
        def _():
            with jax.named_scope("p2_m"):
                make_m(K - 1)
                q_store(K - 1).wait()
        with jax.named_scope("p2_huwait"):
            h_load(s).wait()
            u_load(s).wait()

        @pl.when(s < STEPS - 1)
        def _():
            h_load(s + 1).start()
            u_load(s + 1).start()

        @pl.when(s == STEPS - 1)
        def _():
            next_loads(0)

        @pl.when(s >= 2)
        def _():
            p_store(s - 2).wait()
            for k in PAIR:
                swap(0, s - 2, k).wait_send()
            slot_wait()
        with jax.named_scope("p2_dot"):
            for k in PAIR:
                cc = pl.ds(pl.multiple_of((alt(s)) * FH + k * DQ, DQ), DQ)
                v = jnp.dot(b1[alt(s)], w3g[:, k * DQ:(k + 1) * DQ], preferred_element_type=F32)
                u = acc1[:, cc]
                sig = jax.nn.sigmoid(u)
                q = u * sig
                b0[alt(s), :, quart(k)] = (q * v).astype(BF16)
                acc3[:, cc] = v * sig * (1.0 + u * (1.0 - sig))
                acc1[:, cc] = q
                if k:
                    swap(0, s, 0).start()
        swap(0, s, 1).start()
        q_store(s).start()
        p_store(s).start()
        @pl.when(K >= 1)
        def _():
            with jax.named_scope("p2_dw2"):
                add_dw2(K - 1)
        dyq_load(s).start()
        with jax.named_scope("p2_rsp"):
            rs_proc(K)
    loop(STEPS, pass2)
    for d in own_w:
        d.wait()
    q_store(STEPS - 1).wait()
    for s in (STEPS - 2, STEPS - 1):
        p_store(s).wait()

    with jax.named_scope("w2_wait"):
        for k in TRIO:
            wcopy(2, k).wait_recv()

    def st_copy(k, s):
        return rc(pst.at[s], pstr.at[k, s], ss.at[k], sr.at[k, s], (XP, XC, CP)[k])

    def dx_step(s):
        for k in TRIO:
            st_copy(k, s).wait_recv()
        tot = pst[s] + pstr[0, s] + pstr[1, s] + pstr[2, s]
        mat = jnp.concatenate([tot, jnp.zeros((120, 128), F32)], axis=0).T
        m1 = mat[:, 0:1] * INV_DM
        m2 = mat[:, 1:2] * INV_DM
        inv = st[s, :, 1:2]
        xh = (xown[s].astype(F32) - st[s, :, 0:1]) * inv
        ev = dhs[s % 4] * gsrc[0:1, :]
        dx_ref[s] = (dyown[s].astype(F32) + inv * (ev - m1 - xh * m2)).astype(BF16)

    def pass3(i):
        K = i + STEPS
        s = i
        n = i - 1
        busy = (n >= 0) & (n < STEPS)

        @pl.when(s == 0)
        def _():
            make_m(STEPS - 1)

        @pl.when(busy)
        def _():
            with jax.named_scope("p3_dload"):
                for w in PAIR:
                    for k in PAIR:
                        swap(w, n, k).wait_recv()
            with jax.named_scope("p3_dh"):
                dh = jnp.zeros((TOK, DQ), F32)
                for j in range(4):
                    left = (b0, b1)[j // 2][alt(n), :, (j % 2) * FH:(j % 2 + 1) * FH]
                    dh = dh + lax.dot_general(left, w1g[j * DQ:(j + 1) * DQ, :], NT, preferred_element_type=F32)
                rs_put(STEPS + n, dh)
            rs_first(STEPS + n)

        @pl.when(s < STEPS)
        def _():
            with jax.named_scope("p3_ldwait"):
                for d in block_loads(1, s, dyb, xld) + qp_loads(s):
                    d.wait()

            for k in PAIR:
                swap(0, s, k).wait_send()

            @pl.when(s >= 2)
            def _():
                for k in PAIR:
                    swap(1, s, k).wait_send()
            slot_wait()
            with jax.named_scope("p3_da"):
                for k in PAIR:
                    cc = quart(k)
                    kk = slice(k * DQ, (k + 1) * DQ)
                    da = lax.dot_general(dyb[...], w2g[kk, :], NT, preferred_element_type=F32)
                    b0[alt(s), :, cc] = (da * vb[:, kk]).astype(BF16)
                    b1[alt(s), :, cc] = (da * ub[:, kk]).astype(BF16)
                    if k:
                        swap(0, s, 0).start()
                        swap(1, s, 0).start()
            swap(0, s, 1).start()
            swap(1, s, 1).start()

            @pl.when(s < STEPS - 1)
            def _():
                with jax.named_scope("p3_nextl"):
                    next_loads(s + 1)
        @pl.when(s == 0)
        def _():
            add_dw2(STEPS - 1)
            zero(acc1)
            zero(acc3)

        @pl.when(busy)
        def _():
            w_load(n).wait()
            with jax.named_scope("p3_dw"):
                hqt[...] = hq[...].T
                acc1[...] += jnp.dot(hqt[...], b0[alt(n)], preferred_element_type=F32)
                acc3[...] += jnp.dot(hqt[...], b1[alt(n)], preferred_element_type=F32)

            @pl.when(n < STEPS - 2)
            def _():
                slot_free()

        @pl.when(s < STEPS)
        def _():
            w_load(s).start()

        @pl.when(s < STEPS - DIRECT)
        def _():
            with jax.named_scope("p3_cross"):
                dy_cross(s + DIRECT)

        @pl.when(s >= 4)
        def _():
            for k in TRIO:
                st_copy(k, s - 4).start()

        @pl.when(s >= 5)
        def _():
            with jax.named_scope("p3_dx"):
                dx_step(s - 5)
        with jax.named_scope("p3_rsp"):
            rs_proc(K)
    loop(STEPS + 3, pass3)

    for k in TRIO:
        st_copy(k, STEPS - 1).start()

    def dg_copy(k):
        return rc(dgs, dgr.at[k], dgss.at[k], dgsr.at[k], (YP, ZP, YZ)[k])
    for k in TRIO:
        dg_copy(k).start()

    with jax.named_scope("t_dx"):
        for s in (STEPS - 2, STEPS - 1):
            dx_step(s)
    with jax.named_scope("t_dg"):
        for k in TRIO:
            dg_copy(k).wait_recv()
    tot = dgs[...] + dgr[0] + dgr[1] + dgr[2]
    dg_ref[...] = jnp.broadcast_to(jnp.sum(tot, axis=0, keepdims=True), (8, DQ))

    with jax.named_scope("t_out"):
        for s in (STEPS - 2, STEPS - 1):
            for w in PAIR:
                for k in PAIR:
                    swap(w, s, k).wait_send()
    with jax.named_scope("t_drain"):
        for kind in (X, YA, YB, YBF, ZA, ZB, ZAF):
            wait_bytes(xown, gs.at[0, kind])
        for arr in PAIR:
            for kind in (C0, C1):
                wait_bytes(xg.at[0], gs.at[arr, kind])
        for kind in (YA, ZA):
            wait_bytes(xown, gs.at[1, kind])
        for kind in (X, YB, YBF, ZB):
            wait_bytes(xown.at[0:DIRECT], gs.at[1, kind])
        wait_bytes(xown.at[0:N_YAF], gs.at[1, YAF])
        wait_bytes(xown.at[N_YAF:], gs.at[1, ZAF])
        wait_bytes(xg.at[0, DIRECT:], gs.at[1, XR])
        for k in TRIO:
            wait_bytes(pst, ss.at[k])
            gaincopy(k).wait_send()
            dg_copy(k).wait_send()
            for w in TRIO:
                wcopy(w, k).wait_send()


def finish(y_in, dx_in, dw1_in, dw3_in, dw2_in, dg_in, y_ref, dx_ref, dw1_ref, dw3_ref, dw2_ref, dg_ref, dw2_out, sem):
    outs = [pltpu.make_async_copy(src, dst, sem.at[k]) for k, (src, dst) in enumerate(
        ((dw1_in, dw1_ref), (dw3_in, dw3_ref), (y_in, y_ref), (dx_in, dx_ref)))]
    for d in outs:
        d.start()
    dg_ref[...] = dg_in[0:1, :]
    for i in range(4):
        cols = slice(i * DQ, (i + 1) * DQ)
        dw2_out[cols, :] = dw2_in[:, cols].T
        d = pltpu.make_async_copy(dw2_out.at[cols, :], dw2_ref.at[cols, :], sem.at[4 + i])
        d.start()
        outs.append(d)
    for d in outs:
        d.wait()


def solution(mesh):
    any_spec = pl.BlockSpec(memory_space=pl.ANY)
    vmem_spec = pl.BlockSpec(memory_space=pltpu.VMEM)
    sd = jax.ShapeDtypeStruct
    vm = pltpu.VMEM
    dma = pltpu.SemaphoreType.DMA
    d2, d3 = dma((2,)), dma((3,))

    def local_step(x_blk, dy_blk, gain_blk, w_gate_blk, w_up_blk, w_down_blk):
        outs = pl.pallas_call(
            kernel,
            out_shape=[
                vm((STEPS, ROWS, DQ), BF16), vm((STEPS, ROWS, DQ), BF16),
                vm((DQ, FB), F32), vm((DQ, FB), F32), vm((DQ, FB), F32), vm((8, DQ), F32),
                sd((4, STEPS, TOK, DQ), BF16), sd((4, STEPS, TOK, DQ), BF16),
                sd((STEPS, TOK, DM), BF16), sd((STEPS, TOK, FH), F32), sd((STEPS, TOK, FH), F32),
            ],
            in_specs=[any_spec, any_spec, vmem_spec, any_spec, any_spec, any_spec],
            out_specs=[vmem_spec] * 6 + [any_spec] * 5,
            scratch_shapes=[
                pltpu.VMEM((DM, FH), BF16), pltpu.VMEM((DM, FH), BF16), pltpu.VMEM((FH, DM), BF16),
                pltpu.VMEM((FB, DQ), BF16),
                pltpu.VMEM((2, TOK, FB), BF16), pltpu.VMEM((2, TOK, FB), BF16),
                pltpu.VMEM((TOK, DM), BF16),
                pltpu.VMEM((TOK, FH), F32), pltpu.VMEM((TOK, FH), F32),
                pltpu.VMEM((TOK, DQ), BF16), pltpu.VMEM((DQ, TOK), BF16),
                pltpu.VMEM((STEPS, ROWS, DQ), BF16), pltpu.VMEM((STEPS, ROWS, DQ), BF16),
                pltpu.VMEM((3, 2, 2, 2, ROWS, 256), F32),
                pltpu.VMEM((3, 2, 2, ROWS, 256), F32), pltpu.VMEM((3, 2, ROWS, 256), F32),
                pltpu.VMEM((8, DM), F32), pltpu.VMEM((8, DQ), F32),
                pltpu.VMEM((STEPS, ROWS, 128), F32), pltpu.VMEM((TOK, 128), F32),
                pltpu.VMEM((4, ROWS, DQ), F32),
                pltpu.VMEM((STEPS, 8, 128), F32), pltpu.VMEM((3, STEPS, 8, 128), F32),
                pltpu.VMEM((8, DQ), F32), pltpu.VMEM((3, 8, DQ), F32),
                dma((2, 11)), dma((2, 6, STEPS)), dma((3, 3)), dma((3, 3)), d3, d3,
                dma((2, 2, 2)), dma((2, 2, 2)), dma((4, 4)), dma((4, 4)),
                d3, dma((3, STEPS)), d3, d3,
                dma((8,)), dma((1,)), d2, d2, d2, d2, d2, d2,
                d2, dma((4,)), pltpu.SemaphoreType.REGULAR,
            ],
            compiler_params=pltpu.CompilerParams(collective_id=0, has_side_effects=True,
                                                 vmem_limit_bytes=67043328 - 14 * 2**20 - 2**16),
        )(x_blk.reshape(STEPS, ROWS, DQ), dy_blk.reshape(STEPS, ROWS, DQ), gain_blk.reshape(1, DQ),
          w_gate_blk, w_up_blk, w_down_blk)
        y_blk, dx_blk, dw1, dw3, dw2, dg = pl.pallas_call(
            finish,
            out_shape=[sd((STEPS, ROWS, DQ), BF16), sd((STEPS, ROWS, DQ), BF16), sd((DQ, FB), F32), sd((DQ, FB), F32),
                       sd((FB, DQ), F32), sd((1, DQ), F32)],
            in_specs=[vmem_spec] * 6,
            out_specs=[any_spec] * 5 + [vmem_spec],
            scratch_shapes=[pltpu.VMEM((FB, DQ), F32), dma((8,))],
            compiler_params=pltpu.CompilerParams(vmem_limit_bytes=20 * 2**20),
        )(*outs[:6])
        return (y_blk.reshape(STEPS * ROWS, DQ), dx_blk.reshape(STEPS * ROWS, DQ), dw1, dw3, dw2, dg.reshape(DQ))

    return jax.shard_map(
        local_step, mesh=mesh,
        in_specs=(P("ty", "tx"), P("ty", "tx"), P("tx"), P("tx", "ty"), P("tx", "ty"), P("ty", "tx")),
        out_specs=(P("ty", "tx"), P("ty", "tx"), P("tx", "ty"), P("tx", "ty"), P("ty", "tx"), P("tx")),
        check_vma=False)
```

```python
import jax
import jax.numpy as jnp
from jax import lax
from jax.experimental import pallas as pl
from jax.experimental.pallas import tpu as pltpu
from jax.sharding import PartitionSpec as P

LN_EPS = 1e-6
MESH = pl.DeviceIdType.MESH
BF16 = jnp.bfloat16
F32 = jnp.float32
STEPS = 8
ROWS = 128
TOK = 4 * ROWS
DQ = 512
DM = 4 * DQ
FB = 2048
FH = FB // 2
NT = (((1,), (1,)), ((), ()))
INV_DM = 1.0 / DM
PAIR, TRIO = range(2), range(3)
X, YA, YB, YBF, ZA, ZB, ZAF, C0, C1, YAF, XR, ZBF = range(12)
RECV = [0, 1, 2, 2, 3, 4, 3, 5, 5, 1, 0, 4]
DIRECT = 2
DX_LAG = 6
DX_SLOTS = DX_LAG - 2
N_RS = 2 * STEPS
N_YAF = (STEPS - DIRECT + 1) // 2


def alt(n):
    return n % 2


def kernel(x_ref, dy_ref, g_ref, wg_ref, wu_ref, wd_ref,
           y_ref, dx_ref, acc1, acc3, acc2, dg_ref,
           xg, dyg, hg, ug, vg,
           w1g, w3g, w2g, w2o, b0, b1, dyb, ub, vb,
           hq, hqt, xown, dyown, part, r1, r2, gfull, gsrc, st, stall, dhs,
           pst, pstr, dgs, dgr,
           gs, gr, ws, wr, ggs, ggr, cs, cr, rss, rsr, ss, sr, dgss, dgsr, loc, hst, ust, qst, pstm, hld, uld, ald,
           dld, xld, credit):
    ty = lax.axis_index("ty")
    tx = lax.axis_index("tx")
    y = ty % 2
    z = ty // 2
    c = tx % 2
    tx2 = (tx + 2) % 4
    ty_y = ty + 1 - 2 * y
    ty_z = (ty + 2) % 4
    XP = (ty, tx2)
    CP = (ty, tx + 1 - 2 * c)
    XC = (ty, tx2 + 1 - 2 * c)
    YP = (ty_y, tx)
    ZP = (ty_z, tx)
    YZ = (ty_z + 1 - 2 * y, tx)

    def rc(src, dst, s, r, dev):
        return pltpu.make_async_remote_copy(src_ref=src, dst_ref=dst, send_sem=s, recv_sem=r,
                                            device_id=dev, device_id_type=MESH)

    def lc(src, dst, s):
        return pltpu.make_async_copy(src, dst, s)

    def row(j):
        return pl.ds(pl.multiple_of(j * ROWS, ROWS), ROWS)

    def qcol(q):
        return pl.ds(pl.multiple_of(q * DQ, DQ), DQ)

    def hcol(h):
        return pl.ds(pl.multiple_of(h * FH, FH), FH)

    def gcopy(arr, kind, s):
        own, buf = ((x_ref, xg), (dy_ref, dyg))[arr]
        a, b = gs.at[arr, kind], gr.at[arr, RECV[kind], s]
        if kind in (X, YA, ZA):
            return rc(own.at[s], buf.at[tx, s, row(ty)], a, b, {X: XP, YA: YP, ZA: ZP}[kind])
        if kind in (YB, ZB):
            blk = buf.at[tx2, s, row(ty)]
            return rc(blk, blk, a, b, YP if kind == YB else ZP)
        if kind in (ZAF, YAF, YBF, ZBF):
            to_z = kind in (ZAF, ZBF)
            blk = buf.at[tx2 if kind in (YBF, ZBF) else tx, s, row(ty_y if to_z else ty_z)]
            return rc(blk, blk, a, b, ZP if to_z else YP)
        blk = buf.at[tx2 if kind == C1 else tx, s]
        return rc(blk, blk, a, b, XP if kind == XR else CP)

    def wait_bytes(ref, sem):
        lc(ref, ref, sem).wait()

    def pair_wait(arr, kind, s):
        wait_bytes(xg.at[0, s, 0:2 * ROWS], gr.at[arr, RECV[kind], s])

    def loop(n, f):
        def body(s, carry):
            f(s)
            return carry
        lax.fori_loop(0, n, body, 0)

    def wcopy(w, k):
        dev, h = ((XP, c), (XC, 1 - c), (CP, 1 - c))[k]
        a, b = ws.at[w, k], wr.at[w, k]
        if w < 2:
            return rc((wg_ref, wu_ref)[w].at[:, hcol(h)], (w1g, w3g)[w].at[qcol(tx), :], a, b, dev)
        return rc(wd_ref.at[hcol(h), :], w2g.at[:, qcol(tx)], a, b, dev)

    def gaincopy(k):
        return rc(gsrc, gfull.at[:, qcol(tx)], ggs.at[k], ggr.at[k], (XP, XC, CP)[k])

    gsrc[...] = jnp.broadcast_to(g_ref[...], (8, DQ))
    barrier = pltpu.get_barrier_semaphore()
    for dev in (XP, CP, XC, YP, ZP, YZ):
        pl.semaphore_signal(barrier, inc=1, device_id=dev, device_id_type=MESH)
    own_in = [lc(x_ref, xown, loc.at[0]), lc(dy_ref, dyown, loc.at[1])]
    w_in = [lc(wd_ref, w2o, loc.at[4]),
            lc(wg_ref.at[:, hcol(c)], w1g.at[qcol(tx), :], loc.at[5]),
            lc(wu_ref.at[:, hcol(c)], w3g.at[qcol(tx), :], loc.at[6]),
            lc(wd_ref.at[hcol(c), :], w2g.at[:, qcol(tx)], loc.at[7])]
    for d in own_in:
        d.start()
    with jax.named_scope("barrier"):
        pl.semaphore_wait(barrier, 6)

    for k in TRIO:
        gaincopy(k).start()
    loop(STEPS, lambda s: gcopy(0, X, s).start())

    def send_a(s):
        gcopy(0, YA, s).start()
        gcopy(0, ZA, s).start()
    loop(STEPS, send_a)
    for w in PAIR:
        for k in TRIO:
            wcopy(w, k).start()
    loop(DIRECT, lambda s: gcopy(1, X, s).start())
    for k in TRIO:
        wcopy(2, k).start()
    for d in w_in:
        d.start()
    for d in own_in:
        d.wait()
    own_out = [lc(xown, xg.at[tx, :, row(ty)], loc.at[0]), lc(dyown, dyg.at[tx, :, row(ty)], loc.at[1])]
    for d in own_out:
        d.start()
    gfull[:, qcol(tx)] = gsrc[...]

    def l1(arr, s):
        gcopy(arr, X, s).wait_recv()
        gcopy(arr, YB, s).start()
        gcopy(arr, ZB, s).start()

    def l1f(arr, s):
        gcopy(arr, YA, s).wait_recv()
        gcopy(arr, ZAF, s).start()

    def dy_forward(s):
        odd = (s >= DIRECT) & (alt(s) == 1)

        @pl.when(odd)
        def _():
            gcopy(1, ZA, s).wait_recv()
            gcopy(1, YAF, s).start()

        @pl.when(jnp.logical_not(odd))
        def _():
            gcopy(1, YA, s).wait_recv()
            gcopy(1, ZAF, s).start()

    def dy_quarter(s):
        odd = (s >= DIRECT) & (alt(s) == 1)

        @pl.when(odd)
        def _():
            pair_wait(1, YA, s)

        @pl.when(jnp.logical_not(odd))
        def _():
            pair_wait(1, ZA, s)
        gcopy(1, C0, s).start()

        @pl.when(s >= DIRECT)
        def _():
            gcopy(1, XR, s).start()

    def dy_l2(s):
        @pl.when(s == 1)
        def _():
            gcopy(1, YB, s).wait_recv()
            gcopy(1, ZBF, s).start()

        @pl.when(s != 1)
        def _():
            l2(1, s)

    def dy_rest(s):
        @pl.when(s == 1)
        def _():
            pair_wait(1, ZB, s)

        @pl.when(s != 1)
        def _():
            pair_wait(1, YB, s)
        gcopy(1, C1, s).start()

    def dy_cross(s):
        gcopy(1, XR, s).wait_recv()
        gcopy(1, C1, s).start()

    def l2(arr, s):
        gcopy(arr, ZB, s).wait_recv()
        gcopy(arr, YBF, s).start()

    def l3(arr, s):
        pair_wait(arr, ZA, s)
        gcopy(arr, C0, s).start()
        pair_wait(arr, YB, s)
        gcopy(arr, C1, s).start()

    def first(s):
        l1(0, s)
        l1f(0, s)
    with jax.named_scope("g_first"):
        loop(STEPS, first)
    with jax.named_scope("g_l2"):
        loop(STEPS, lambda s: l2(0, s))

    def send_dya(s):
        gcopy(1, YA, s).start()
        gcopy(1, ZA, s).start()
    loop(STEPS, send_dya)
    with jax.named_scope("g_local"):
        for d in own_out:
            d.wait()
        for d in w_in:
            d.wait()
        for k in TRIO:
            gaincopy(k).wait_recv()
    with jax.named_scope("g_l3"):
        loop(STEPS, lambda s: l3(0, s))

    def block_loads(arr, s, dst, sem):
        buf = (xg, dyg)[arr]
        return [lc(buf.at[q, s], dst.at[:, q * DQ:(q + 1) * DQ], sem.at[q]) for q in range(4)]

    def wait_block(arr, s):
        wait_bytes(xg.at[0:2, s], gr.at[arr, RECV[C0], s])

    xs, hb = b1.at[0], b1.at[1]

    def h_store(s):
        return lc(hb, hg.at[s], hst.at[0])

    def u_store(s):
        return lc(acc2.at[:, hcol(alt(s))], ug.at[s], ust.at[alt(s)])

    wait_block(0, 0)
    for d in block_loads(0, 0, xs, xld):
        d.start()
    with jax.named_scope("w1_wait"):
        for k in TRIO:
            wcopy(0, k).wait_recv()

    def pass1(s):
        with jax.named_scope("p1_xwait"):
            for d in block_loads(0, s, xs, xld):
                d.wait()

        @pl.when(s >= 1)
        def _():
            h_store(s - 1).wait()

        def chunk(i):
            rr = pl.ds(pl.multiple_of(i * 64, 64), 64)
            xf = xs[rr, :].astype(F32)
            mu = jnp.sum(xf, axis=1, keepdims=True) * INV_DM
            sq = jnp.sum(xf * xf, axis=1, keepdims=True) * INV_DM
            inv = lax.rsqrt(sq - mu * mu + LN_EPS)
            hb[rr, :] = (gfull[0:1, :] * ((xf - mu) * inv)).astype(BF16)
            lane = lax.broadcasted_iota(jnp.int32, (64, 128), 1)
            stall[rr, :] = jnp.where(lane == 0, mu, inv)
        with jax.named_scope("p1_ln"):
            loop(TOK // 64, chunk)
        st[s] = stall[row(ty), :]
        h_store(s).start()

        @pl.when(s < STEPS - 1)
        def _():
            wait_block(0, s + 1)
            for d in block_loads(0, s + 1, xs, xld):
                d.start()

        @pl.when(s >= 2)
        def _():
            u_store(s - 2).wait()
        with jax.named_scope("p1_dot"):
            acc2[:, hcol(alt(s))] = jnp.dot(hb[...], w1g[...], preferred_element_type=F32)
        u_store(s).start()
        with jax.named_scope("p1_fwd"):
            dy_forward(s)
    loop(STEPS, pass1)
    h_store(STEPS - 1).wait()
    u_store(STEPS - 2).wait()
    u_store(STEPS - 1).wait()

    def rs_copy(kind, n):
        slot = n % 3
        a, b = rss.at[kind, n % 4], rsr.at[kind, n % 4]
        if kind == 0:
            return rc(part.at[slot, 0, 1 - y], r1.at[n % 3, 0], a, b, YP)
        if kind == 1:
            return rc(part.at[slot, 1, 1 - z], r1.at[n % 3, 1], a, b, ZP)
        if kind == 2:
            return rc(part.at[slot, 0, y, 1 - z], r2.at[n % 3, 0], a, b, ZP)
        return rc(part.at[slot, 1, z, 1 - y], r2.at[n % 3, 1], a, b, YP)

    def rs_put(n, val):
        slot = n % 3
        for j in range(4):
            part[slot, 0, j % 2, j // 2] = val[j * ROWS:(j + 1) * ROWS, 0:256]
            part[slot, 1, j // 2, j % 2] = val[j * ROWS:(j + 1) * ROWS, 256:512]

    def rs_first(n):
        rs_copy(0, n).start()
        rs_copy(1, n).start()

    def rs_proc(K):
        @pl.when((K >= 2) & (K < N_RS + 2))
        def _():
            n = K - 2
            slot = n % 3
            for k in PAIR:
                rs_copy(k, n).wait_recv()
            for k in PAIR:
                part[slot, 0, y, k] += r1[slot, 0, k]
                part[slot, 1, z, k] += r1[slot, 1, k]
            rs_copy(2, n).start()
            rs_copy(3, n).start()

        @pl.when(K >= 3)
        def _():
            n = K - 3
            slot = n % 3
            for k in PAIR:
                rs_copy(2 + k, n).wait_recv()
            m0, m1 = r2[slot, 0], r2[slot, 1]
            for k in range(4):
                rs_copy(k, n).wait_send()

            @pl.when(n < 8)
            def _():
                y_ref[n, :, 0:256] = (xown[n, :, 0:256].astype(F32) + (part[slot, 0, y, z] + m0)).astype(BF16)
                y_ref[n, :, 256:512] = (xown[n, :, 256:512].astype(F32) + (part[slot, 1, z, y] + m1)).astype(BF16)

            @pl.when(n >= 8)
            def _():
                s = n - 8
                dhs[s % DX_SLOTS, :, 0:256] = part[slot, 0, y, z] + m0
                dhs[s % DX_SLOTS, :, 256:512] = part[slot, 1, z, y] + m1
                dh = dhs[s % DX_SLOTS]
                xh = (xown[s].astype(F32) - st[s, :, 0:1]) * st[s, :, 1:2]
                ev = dh * gsrc[0:1, :]
                dgs[...] += jnp.sum((dh * xh).reshape(ROWS // 8, 8, DQ), axis=0)
                s1 = jnp.sum(ev, axis=1, keepdims=True)
                s2 = jnp.sum(ev * xh, axis=1, keepdims=True)
                lane = lax.broadcasted_iota(jnp.int32, (ROWS, 128), 1)
                mat = jnp.where(lane == 0, s1, jnp.where(lane == 1, s2, 0.0))
                pst[s] = mat.T[0:8, :]

    def h_load(s):
        return lc(hg.at[s], b1.at[alt(s)], hld.at[alt(s)])

    def u_load(s):
        return lc(ug.at[s], acc1.at[:, hcol(alt(s))], uld.at[alt(s)])

    def q_store(s):
        return lc(acc1.at[:, hcol(alt(s))], ug.at[s], qst.at[alt(s)])

    def p_store(s):
        return lc(acc3.at[:, hcol(alt(s))], vg.at[s], pstm.at[alt(s)])

    def quart(k):
        return pl.ds(pl.multiple_of(c * FH + k * DQ, DQ), DQ)

    def swap(buf, s, k):
        blk = (b0, b1)[buf].at[alt(s), :, quart(k)]
        return rc(blk, blk, cs.at[buf, alt(s), k], cr.at[buf, alt(s), k], CP)

    def slot_free():
        pl.semaphore_signal(credit, inc=1, device_id=CP, device_id_type=MESH)

    def slot_wait():
        pl.semaphore_wait(credit, 1)

    def dyq_load(s):
        return lc(dyg.at[tx, s], hq, ald.at[1])

    def make_m(n):
        for k in PAIR:
            swap(0, n, k).wait_recv()
        rs_put(n, jnp.dot(b0[alt(n)], w2o[...], preferred_element_type=F32))
        rs_first(n)

    def add_dw2(n):
        dyq_load(n).wait()
        hqt[...] = hq[...].T
        acc2[...] += jnp.dot(hqt[...], b0[alt(n)], preferred_element_type=F32)
        slot_free()

    def zero(acc):
        def body(j):
            acc[pl.ds(pl.multiple_of(j * 16, 16), 16), :] = jnp.zeros((16, FB), F32)
        loop(DQ // 16, body)

    def qp_loads(s):
        return [lc(ug.at[s], ub, dld.at[0]), lc(vg.at[s], vb, dld.at[1])]

    def w_load(s):
        return lc(hg.at[s, :, qcol(tx)], hq, ald.at[0])

    def next_loads(s):
        wait_block(1, s)
        for d in block_loads(1, s, dyb, xld) + qp_loads(s):
            d.start()

    zero(acc2)
    h_load(0).start()
    u_load(0).start()
    dgs[...] = jnp.zeros_like(dgs)
    last = tx2 + 1 - 2 * c
    for k in (2, 0):
        wcopy(1, k).wait_recv()
    h_load(0).wait()
    acc3[:, 0:FH] = sum(jnp.dot(b1[0, :, qcol(q)], w3g[qcol(q), :], preferred_element_type=F32)
                        for q in (tx, tx + 1 - 2 * c, tx2))
    with jax.named_scope("w3_wait"):
        wcopy(1, 1).wait_recv()

    own_w = [lc(w.at[:, hcol(h)], w1g.at[qcol(2 * k + h), :], loc.at[2 * k + h])
             for k, w in enumerate((wg_ref, wu_ref)) for h in PAIR]
    for d in own_w:
        d.start()

    def pass2(K):
        s = K
        with jax.named_scope("p2_comm"):
            dy_quarter(K)

            @pl.when((K >= 1) & (K <= DIRECT))
            def _():
                l1(1, K - 1)

            @pl.when((K >= 3) & (K <= 2 + DIRECT))
            def _():
                dy_l2(K - 3)

            @pl.when((K >= 5) & (K <= 4 + DIRECT))
            def _():
                dy_rest(K - 5)

        @pl.when(K >= 1)
        def _():
            with jax.named_scope("p2_m"):
                make_m(K - 1)
                q_store(K - 1).wait()
        with jax.named_scope("p2_huwait"):
            @pl.when(s > 0)
            def _():
                h_load(s).wait()
            u_load(s).wait()

        @pl.when(s < STEPS - 1)
        def _():
            h_load(s + 1).start()
            u_load(s + 1).start()

        @pl.when(s == STEPS - 1)
        def _():
            next_loads(0)

        @pl.when(s >= 2)
        def _():
            p_store(s - 2).wait()
            for k in PAIR:
                swap(0, s - 2, k).wait_send()
            slot_wait()
        def gate(k, v):
            cc = pl.ds(pl.multiple_of(alt(s) * FH + k * DQ, DQ), DQ)
            u = acc1[:, cc]
            sig = jax.nn.sigmoid(u)
            q = u * sig
            b0[alt(s), :, quart(k)] = (q * v).astype(BF16)
            acc3[:, cc] = v * sig * (1.0 + u * (1.0 - sig))
            acc1[:, cc] = q
            if k:
                swap(0, s, 0).start()

        @pl.when(s > 0)
        def _():
            with jax.named_scope("p2_dot"):
                for k in PAIR:
                    gate(k, jnp.dot(b1[alt(s)], w3g[:, k * DQ:(k + 1) * DQ], preferred_element_type=F32))

        @pl.when(s == 0)
        def _():
            with jax.named_scope("p2_dot0"):
                for k in PAIR:
                    kk = slice(k * DQ, (k + 1) * DQ)
                    gate(k, acc3[:, kk] + jnp.dot(b1[0, :, qcol(last)], w3g[qcol(last), kk], preferred_element_type=F32))
        swap(0, s, 1).start()
        q_store(s).start()
        p_store(s).start()
        @pl.when(K >= 1)
        def _():
            with jax.named_scope("p2_dw2"):
                add_dw2(K - 1)
        dyq_load(s).start()
        with jax.named_scope("p2_rsp"):
            rs_proc(K)
    loop(STEPS, pass2)
    for d in own_w:
        d.wait()
    q_store(STEPS - 1).wait()
    for s in (STEPS - 2, STEPS - 1):
        p_store(s).wait()

    with jax.named_scope("w2_wait"):
        for k in TRIO:
            wcopy(2, k).wait_recv()

    def st_copy(k, s):
        return rc(pst.at[s], pstr.at[k, s], ss.at[k], sr.at[k, s], (XP, XC, CP)[k])

    def dx_step(s):
        for k in TRIO:
            st_copy(k, s).wait_recv()
        tot = pst[s] + pstr[0, s] + pstr[1, s] + pstr[2, s]
        mat = jnp.concatenate([tot, jnp.zeros((120, 128), F32)], axis=0).T
        m1 = mat[:, 0:1] * INV_DM
        m2 = mat[:, 1:2] * INV_DM
        inv = st[s, :, 1:2]
        xh = (xown[s].astype(F32) - st[s, :, 0:1]) * inv
        ev = dhs[s % DX_SLOTS] * gsrc[0:1, :]
        dx_ref[s] = (dyown[s].astype(F32) + inv * (ev - m1 - xh * m2)).astype(BF16)

    def pass3(i):
        K = i + STEPS
        s = i
        n = i - 1
        busy = (n >= 0) & (n < STEPS)

        @pl.when(s == 0)
        def _():
            make_m(STEPS - 1)

        @pl.when(busy)
        def _():
            with jax.named_scope("p3_dload"):
                for w in PAIR:
                    for k in PAIR:
                        swap(w, n, k).wait_recv()
            with jax.named_scope("p3_dh"):
                dh = jnp.zeros((TOK, DQ), F32)
                for j in range(4):
                    left = (b0, b1)[j // 2][alt(n), :, (j % 2) * FH:(j % 2 + 1) * FH]
                    dh = dh + lax.dot_general(left, w1g[j * DQ:(j + 1) * DQ, :], NT, preferred_element_type=F32)
                rs_put(STEPS + n, dh)
            rs_first(STEPS + n)

        @pl.when((s >= DIRECT - 1) & (s < STEPS - 1))
        def _():
            with jax.named_scope("p3_cross"):
                dy_cross(s + 1)

        @pl.when(s < STEPS)
        def _():
            with jax.named_scope("p3_ldwait"):
                for d in block_loads(1, s, dyb, xld) + qp_loads(s):
                    d.wait()

            for k in PAIR:
                swap(0, s, k).wait_send()

            @pl.when(s >= 2)
            def _():
                for k in PAIR:
                    swap(1, s, k).wait_send()
            slot_wait()
            with jax.named_scope("p3_da"):
                for k in PAIR:
                    cc = quart(k)
                    kk = slice(k * DQ, (k + 1) * DQ)
                    da = lax.dot_general(dyb[...], w2g[kk, :], NT, preferred_element_type=F32)
                    b0[alt(s), :, cc] = (da * vb[:, kk]).astype(BF16)
                    b1[alt(s), :, cc] = (da * ub[:, kk]).astype(BF16)
                    if k:
                        swap(0, s, 0).start()
                        swap(1, s, 0).start()
            swap(0, s, 1).start()
            swap(1, s, 1).start()

        @pl.when(s == 0)
        def _():
            add_dw2(STEPS - 1)
            zero(acc1)
            zero(acc3)

        @pl.when(busy)
        def _():
            w_load(n).wait()
            with jax.named_scope("p3_dw"):
                hqt[...] = hq[...].T
                acc1[...] += jnp.dot(hqt[...], b0[alt(n)], preferred_element_type=F32)
                acc3[...] += jnp.dot(hqt[...], b1[alt(n)], preferred_element_type=F32)

            @pl.when(n < STEPS - 2)
            def _():
                slot_free()

        @pl.when(s < STEPS)
        def _():
            w_load(s).start()

        @pl.when(s < STEPS - 1)
        def _():
            with jax.named_scope("p3_nextl"):
                next_loads(s + 1)

        @pl.when(s >= 4)
        def _():
            for k in TRIO:
                st_copy(k, s - 4).start()

        @pl.when(s >= DX_LAG)
        def _():
            with jax.named_scope("p3_dx"):
                dx_step(s - DX_LAG)
        with jax.named_scope("p3_rsp"):
            rs_proc(K)
    loop(STEPS + 3, pass3)

    for k in TRIO:
        st_copy(k, STEPS - 1).start()

    def dg_copy(k):
        return rc(dgs, dgr.at[k], dgss.at[k], dgsr.at[k], (YP, ZP, YZ)[k])
    for k in TRIO:
        dg_copy(k).start()

    with jax.named_scope("t_dx"):
        loop(DX_LAG - 3, lambda s: dx_step(STEPS + 3 - DX_LAG + s))
    with jax.named_scope("t_dg"):
        for k in TRIO:
            dg_copy(k).wait_recv()
    tot = dgs[...] + dgr[0] + dgr[1] + dgr[2]
    dg_ref[...] = jnp.broadcast_to(jnp.sum(tot, axis=0, keepdims=True), (8, DQ))

    with jax.named_scope("t_out"):
        for s in (STEPS - 2, STEPS - 1):
            for w in PAIR:
                for k in PAIR:
                    swap(w, s, k).wait_send()
    with jax.named_scope("t_drain"):
        for kind in (X, YA, YB, YBF, ZA, ZB, ZAF):
            wait_bytes(xown, gs.at[0, kind])
        for arr in PAIR:
            for kind in (C0, C1):
                wait_bytes(xg.at[0], gs.at[arr, kind])
        for kind in (YA, ZA):
            wait_bytes(xown, gs.at[1, kind])
        for kind in (X, YB, ZB):
            wait_bytes(xown.at[0:DIRECT], gs.at[1, kind])
        wait_bytes(xown.at[0:DIRECT - 1], gs.at[1, YBF])
        wait_bytes(xown.at[0], gs.at[1, ZBF])
        wait_bytes(xown.at[0:N_YAF], gs.at[1, YAF])
        wait_bytes(xown.at[N_YAF:], gs.at[1, ZAF])
        wait_bytes(xg.at[0, DIRECT:], gs.at[1, XR])
        for k in TRIO:
            wait_bytes(pst, ss.at[k])
            gaincopy(k).wait_send()
            dg_copy(k).wait_send()
            for w in TRIO:
                wcopy(w, k).wait_send()


def finish(y_in, dx_in, dw1_in, dw3_in, dw2_in, dg_in, y_ref, dx_ref, dw1_ref, dw3_ref, dw2_ref, dg_ref, dw2_out, sem):
    outs = [pltpu.make_async_copy(src, dst, sem.at[k]) for k, (src, dst) in enumerate(
        ((dw1_in, dw1_ref), (dw3_in, dw3_ref), (y_in, y_ref), (dx_in, dx_ref)))]
    for d in outs:
        d.start()
    dg_ref[...] = dg_in[0:1, :]
    for i in range(4):
        cols = slice(i * DQ, (i + 1) * DQ)
        dw2_out[cols, :] = dw2_in[:, cols].T
        d = pltpu.make_async_copy(dw2_out.at[cols, :], dw2_ref.at[cols, :], sem.at[4 + i])
        d.start()
        outs.append(d)
    for d in outs:
        d.wait()


def solution(mesh):
    any_spec = pl.BlockSpec(memory_space=pl.ANY)
    vmem_spec = pl.BlockSpec(memory_space=pltpu.VMEM)
    sd = jax.ShapeDtypeStruct
    vm = pltpu.VMEM
    dma = pltpu.SemaphoreType.DMA
    d2, d3 = dma((2,)), dma((3,))

    def local_step(x_blk, dy_blk, gain_blk, w_gate_blk, w_up_blk, w_down_blk):
        outs = pl.pallas_call(
            kernel,
            out_shape=[
                vm((STEPS, ROWS, DQ), BF16), vm((STEPS, ROWS, DQ), BF16),
                vm((DQ, FB), F32), vm((DQ, FB), F32), vm((DQ, FB), F32), vm((8, DQ), F32),
                sd((4, STEPS, TOK, DQ), BF16), sd((4, STEPS, TOK, DQ), BF16),
                sd((STEPS, TOK, DM), BF16), sd((STEPS, TOK, FH), F32), sd((STEPS, TOK, FH), F32),
            ],
            in_specs=[any_spec, any_spec, vmem_spec, any_spec, any_spec, any_spec],
            out_specs=[vmem_spec] * 6 + [any_spec] * 5,
            scratch_shapes=[
                pltpu.VMEM((DM, FH), BF16), pltpu.VMEM((DM, FH), BF16), pltpu.VMEM((FH, DM), BF16),
                pltpu.VMEM((FB, DQ), BF16),
                pltpu.VMEM((2, TOK, FB), BF16), pltpu.VMEM((2, TOK, FB), BF16),
                pltpu.VMEM((TOK, DM), BF16),
                pltpu.VMEM((TOK, FH), F32), pltpu.VMEM((TOK, FH), F32),
                pltpu.VMEM((TOK, DQ), BF16), pltpu.VMEM((DQ, TOK), BF16),
                pltpu.VMEM((STEPS, ROWS, DQ), BF16), pltpu.VMEM((STEPS, ROWS, DQ), BF16),
                pltpu.VMEM((3, 2, 2, 2, ROWS, 256), F32),
                pltpu.VMEM((3, 2, 2, ROWS, 256), F32), pltpu.VMEM((3, 2, ROWS, 256), F32),
                pltpu.VMEM((8, DM), F32), pltpu.VMEM((8, DQ), F32),
                pltpu.VMEM((STEPS, ROWS, 128), F32), pltpu.VMEM((TOK, 128), F32),
                pltpu.VMEM((DX_SLOTS, ROWS, DQ), F32),
                pltpu.VMEM((STEPS, 8, 128), F32), pltpu.VMEM((3, STEPS, 8, 128), F32),
                pltpu.VMEM((8, DQ), F32), pltpu.VMEM((3, 8, DQ), F32),
                dma((2, 12)), dma((2, 6, STEPS)), dma((3, 3)), dma((3, 3)), d3, d3,
                dma((2, 2, 2)), dma((2, 2, 2)), dma((4, 4)), dma((4, 4)),
                d3, dma((3, STEPS)), d3, d3,
                dma((8,)), dma((1,)), d2, d2, d2, d2, d2, d2,
                d2, dma((4,)), pltpu.SemaphoreType.REGULAR,
            ],
            compiler_params=pltpu.CompilerParams(collective_id=0, has_side_effects=True,
                                                 vmem_limit_bytes=67043328 - 14 * 2**20 - 2**16),
        )(x_blk.reshape(STEPS, ROWS, DQ), dy_blk.reshape(STEPS, ROWS, DQ), gain_blk.reshape(1, DQ),
          w_gate_blk, w_up_blk, w_down_blk)
        y_blk, dx_blk, dw1, dw3, dw2, dg = pl.pallas_call(
            finish,
            out_shape=[sd((STEPS, ROWS, DQ), BF16), sd((STEPS, ROWS, DQ), BF16), sd((DQ, FB), F32), sd((DQ, FB), F32),
                       sd((FB, DQ), F32), sd((1, DQ), F32)],
            in_specs=[vmem_spec] * 6,
            out_specs=[any_spec] * 5 + [vmem_spec],
            scratch_shapes=[pltpu.VMEM((FB, DQ), F32), dma((8,))],
            compiler_params=pltpu.CompilerParams(vmem_limit_bytes=20 * 2**20),
        )(*outs[:6])
        return (y_blk.reshape(STEPS * ROWS, DQ), dx_blk.reshape(STEPS * ROWS, DQ), dw1, dw3, dw2, dg.reshape(DQ))

    return jax.shard_map(
        local_step, mesh=mesh,
        in_specs=(P("ty", "tx"), P("ty", "tx"), P("tx"), P("tx", "ty"), P("tx", "ty"), P("ty", "tx")),
        out_specs=(P("ty", "tx"), P("ty", "tx"), P("tx", "ty"), P("tx", "ty"), P("ty", "tx"), P("tx")),
        check_vma=False)
```
